32 devices in a mesh: grp: 2 (over y), sp: 16 (over z, x, core).
Axes of the slice: x: 2, y: 2, z: 4, core: 2. Of those that a mesh axis runs over, the one named last changes fastest.
Arguments:
- alpha: float32 [20, 16, 4096], P('grp', None, 'sp'), may hold values from -6 to 6
- ensemble: bfloat16 [20, 3, 16, 4096], P('grp', None, None, 'sp'), may hold values from -6 to 6
- static_std: float32 [3, 16, 4096], P(None, 'grp', 'sp'), may hold values from 0.2 to 1
- control: float32 [3, 16, 4096], P(None, 'grp', 'sp'), may hold values from -6 to 6
- loc_spectrum: float32 [1024], replicated, may hold values from 0.00024414062 to 0.001953125
- obs_cell: int32 [32768], P(('grp', 'sp')), may hold values from 0 to 65535, as said below
- obs_step: int32 [32768], P(('grp', 'sp')), may hold values from 0 to 2
- innovation: float32 [32768], P(('grp', 'sp')), may hold values from -6 to 6
- obs_weight: float32 [32768], P(('grp', 'sp')), may hold values from 0.5 to 4
Outputs:
- grad_alpha: float32 [20, 16, 4096], P('grp', None, 'sp')
- grad_control: float32 [3, 16, 4096], P(None, 'grp', 'sp')
The draws below stay inside these ranges and needn't reach their ends.
Inputs may be any that keep to these rules, and one draw needn't show every extreme that they name: `obs_cell`: an entry is row * 4096 + column. Entries 1024 * b to 1024 * (b + 1) - 1 lie in the tile of 8 rows from row 8 * (b // 16) and 256 columns from column 256 * (b % 16).
All inputs are finite; a program needn't handle non-finite values.
Results may differ from the reference program's by a relative error of at most 0.0075.
Values may be sent and summed in bfloat16 or wider, within the bound.
A program may use at most 128 MiB of HBM per device.

```python
import math
import jax
import jax.numpy as jnp
from jax import lax

NX = 4096
KEEP = 1024
STEPS = 2
OBS_DEV = 1024
MEMBERS = 20
NY = 16
TILE_ROWS = 8
TILE_COLS = 256
OBS = 32768


def draw_obs_cell(key, part):
    base = jax.random.fold_in(key, 11)
    row_key, col_key = jax.random.split(base)
    blocks = jnp.arange(OBS, dtype=jnp.int32) // OBS_DEV
    col_blocks = NX // TILE_COLS
    block_row = blocks // col_blocks
    block_col = blocks % col_blocks
    local_row = jax.random.randint(row_key, (OBS,), 0, TILE_ROWS, dtype=jnp.int32)
    local_col = jax.random.randint(col_key, (OBS,), 0, TILE_COLS, dtype=jnp.int32)
    return ((block_row * TILE_ROWS + local_row) * NX + block_col * TILE_COLS + local_col).astype(jnp.int32)


def plant(result, key, low, high):
    spot = [jax.random.randint(jax.random.fold_in(key, axis), (), 0, length) for axis, length in enumerate(result.shape)]
    main_axis = result.shape.index(max(result.shape))
    beside = spot[:main_axis] + [(spot[main_axis] + 1) % result.shape[main_axis]] + spot[main_axis + 1:]
    return result.at[tuple(spot)].set(low).at[tuple(beside)].set(high)


def strengthened(array, rng, source, target, parts, factor):
    def block_of(dim):
        return (jnp.arange(array.shape[dim]) // (array.shape[dim] // parts)).reshape((-1,) + (1,) * (array.ndim - 1 - dim))

    one_side = jax.random.permutation(rng, parts)[block_of(target)]
    other_side = (block_of(target) + parts // 2) % parts
    return jnp.where((block_of(source) == one_side) | (block_of(source) == other_side), factor * array, array)


def block_scale(key, extent, shards, low, high):
    def one(axis_at, blocks):
        draws = jax.random.uniform(jax.random.fold_in(jax.random.fold_in(key, 6), axis_at), (blocks,), jnp.float32, low / len(shards), high / len(shards))
        return jnp.repeat(jnp.exp(draws), extent[axis_at] // blocks).reshape((-1,) + (1,) * (len(extent) - axis_at - 1))

    level = one(*shards[0])
    for cut in shards[1:]:
        level = level * one(*cut)
    return level


def centred(stream_key, shape, scale, limit, pieces=(), kind=jnp.bfloat16):
    drawn = jax.random.normal(stream_key, shape, jnp.float32) * scale
    if len(pieces) > 0:
        drawn = block_scale(stream_key, shape, pieces, -0.22, 0.18) * drawn
    return jnp.clip(drawn, min=-limit, max=limit).astype(kind)


def noise_with(key, dims, scale, limit, pieces, heavy, held_as=jnp.bfloat16):
    array = scale * jax.random.normal(key, dims, jnp.float32)
    if pieces:
        array = array * block_scale(key, dims, pieces, -0.22, 0.18)
    return jnp.clip(strengthened(array, jax.random.fold_in(key, 3), *heavy), -limit, limit).astype(held_as)


def setup_inputs(seed: int = 0) -> dict:
    key_of = jax.random.split(jax.random.key(seed), 10)
    alpha = centred(key_of[0], (MEMBERS, NY, NX), 1.0, 6.0, ((0, 2), (2, 16)), jnp.float32)
    ensemble = noise_with(key_of[1], (MEMBERS, 3, NY, NX), 1.0, 6.0, ((0, 2), (3, 16)), (0, 2, 2, 2.0))
    static_std = jnp.clip(jnp.exp(math.log(1.0) - 1.609438 * jax.random.uniform(key_of[2], (3, NY, NX), jnp.float32) ** block_scale(key_of[2], (3, NY, NX), ((1, 2), (2, 16)), -0.2, 0.2)), 0.2, 1.0)
    control = centred(key_of[3], (3, NY, NX), 1.0, 6.0, ((1, 2), (2, 16)), jnp.float32)
    loc_spectrum = jnp.clip(jnp.exp(jax.random.uniform(key_of[4], (KEEP,), jnp.float32, math.log(0.00024414062), math.log(0.001953125))), 0.00024414062, 0.001953125)
    obs_cell = draw_obs_cell(jax.random.fold_in(key_of[9], 71), 0)
    obs_step = plant(jax.random.randint(key_of[6], (OBS,), 0, STEPS + 1), jax.random.fold_in(key_of[6], 1), 0, STEPS).astype(jnp.int32)
    innovation = centred(key_of[7], (OBS,), 1.0, 6.0, ((0, 32),), jnp.float32)
    obs_weight = jnp.clip(jnp.exp(math.log(4.0) - 2.0794415 * jax.random.uniform(key_of[8], (OBS,), jnp.float32) ** block_scale(key_of[8], (OBS,), ((0, 32),), -0.2, 0.2)), 0.5, 4.0)
    return {"alpha": alpha, "ensemble": ensemble, "static_std": static_std, "control": control, "loc_spectrum": loc_spectrum, "obs_cell": obs_cell, "obs_step": obs_step, "innovation": innovation, "obs_weight": obs_weight}


courant = 0.4

def spectral_filter(rows_data, loc_spectrum):
    length_x = rows_data.shape[1]
    kept_waves = loc_spectrum.shape[0]
    freq_block = math.gcd(kept_waves, 256)
    positions = jnp.arange(length_x, dtype=jnp.int32)
    filtered = jnp.zeros(rows_data.shape, jnp.float32)
    for start_wave in range(0, kept_waves, freq_block):
        waves = start_wave + jnp.arange(freq_block, dtype=jnp.int32)
        phases = positions[:, None] * waves[None, :] % length_x
        radians = 2.0 * math.pi / length_x * phases.astype(jnp.float32)
        fourier_basis = jnp.concatenate([jnp.cos(radians), jnp.sin(radians)], axis=1)
        weights = loc_spectrum[start_wave:start_wave + freq_block]
        weights = jnp.concatenate([weights, weights])
        coeffs = jnp.dot(rows_data, fourier_basis, precision=lax.Precision.HIGHEST, preferred_element_type=jnp.float32)
        filtered = filtered + jnp.dot(coeffs * weights[None, :], fourier_basis.T, precision=lax.Precision.HIGHEST, preferred_element_type=jnp.float32)
    return filtered

def diff_x(field):
    return 0.5 * (jnp.roll(field, -1, axis=-1) - jnp.roll(field, 1, axis=-1))

def diff_y(field):
    padded = jnp.pad(field, ((1, 1), (0, 0)))
    return 0.5 * (padded[2:] - padded[:-2])

def coriolis():
    rows_index = jnp.arange(NY, dtype=jnp.int32).astype(jnp.float32)
    return (0.1 + 0.2 * (rows_index + 0.5) / NY)[:, None]

def model_step(state, rotation):
    height, eastward, northward = (state[0], state[1], state[2])
    new_height = height - courant * (diff_x(eastward) + diff_y(northward))
    new_east = eastward - courant * diff_x(new_height) + rotation * northward
    new_north = northward - courant * diff_y(new_height) - rotation * eastward
    return jnp.stack([new_height, new_east, new_north])

def adjoint_step(state, rotation):
    back_h, back_u, back_w = (state[0], state[1], state[2])
    adj_height = back_h + courant * (diff_x(back_u) + diff_y(back_w))
    adj_east = back_u - rotation * back_w + courant * diff_x(adj_height)
    adj_north = back_w + rotation * back_u + courant * diff_y(adj_height)
    return jnp.stack([adj_height, adj_east, adj_north])

def reference(alpha, ensemble, static_std, control, loc_spectrum, obs_cell, obs_step, innovation, obs_weight):
    spread = 1.0 / math.sqrt(MEMBERS - 1)
    rotation = coriolis()
    localized = spectral_filter(alpha.reshape(MEMBERS * NY, NX), loc_spectrum).reshape(alpha.shape).astype(jnp.bfloat16)
    partial_value = jnp.einsum('mvyx,myx->vyx', ensemble.astype(jnp.float32), localized.astype(jnp.float32), precision=lax.Precision.HIGHEST)
    increment = static_std * control + spread * partial_value
    first_state = model_step(increment, rotation)
    second_state = model_step(first_state, rotation)
    states = (increment, first_state, second_state)
    observed = jnp.zeros(innovation.shape, jnp.float32)
    for moment in range(3):
        values = states[moment][0].reshape(-1)[obs_cell]
        observed = jnp.where(obs_step == moment, values, observed)
    misfit = obs_weight * (observed - innovation)
    zero_field = jnp.zeros((NY, NX), jnp.float32)
    forcings = []
    for moment in range(3):
        spread_obs = jnp.where(obs_step == moment, misfit, jnp.zeros_like(misfit))
        height_force = jnp.zeros((NY * NX,), jnp.float32).at[obs_cell].add(spread_obs).reshape(NY, NX)
        forcings.append(jnp.stack([height_force, zero_field, zero_field]))
    adjoint = adjoint_step(forcings[2], rotation) + forcings[1]
    adjoint = adjoint_step(adjoint, rotation) + forcings[0]
    grad_control = control + static_std * adjoint
    half = adjoint.astype(jnp.bfloat16)
    weighted = jnp.einsum('mvyx,vyx->myx', ensemble.astype(jnp.float32), half.astype(jnp.float32), precision=lax.Precision.HIGHEST)
    grad_alpha = alpha + spread * spectral_filter(weighted.reshape(MEMBERS * NY, NX), loc_spectrum).reshape(alpha.shape)
    return (grad_alpha, grad_control)
```

```python
import math

import jax
import jax.numpy as jnp
import numpy as np
from jax import lax
from jax.sharding import PartitionSpec as P

COURANT = 0.4


def tables(parts, cols, waves):
    length = parts * cols
    inner_waves = waves // parts
    k1 = np.arange(parts)
    turn = 2 * np.pi * (np.outer(k1, np.arange(parts)) % parts) / parts
    outer = np.concatenate([np.cos(turn), -np.sin(turn)])
    twist = 2 * np.pi * np.outer(k1, np.arange(cols)) / length
    phase = 2 * np.pi * (np.outer(np.arange(cols), np.arange(inner_waves)) % cols) / cols
    c, s = np.cos(phase), np.sin(phase)
    inner = np.block([[c, -s], [s, c]])
    return [np.asarray(t, np.float32) for t in (outer, np.cos(twist), np.sin(twist), inner)]


def mul(a, b):
    return jnp.dot(a, b, precision=lax.Precision.HIGH, preferred_element_type=jnp.float32)


def spectral_filter(blocks, loc_spectrum):
    parts, items, cols = blocks.shape
    outer, tw_c, tw_s, inner = tables(parts, cols, loc_spectrum.shape[0])
    tw_c, tw_s = tw_c[:, None, :], tw_s[:, None, :]
    half = inner.shape[1] // 2
    weights = loc_spectrum.reshape(half, parts).T
    weights = jnp.concatenate([weights, weights], axis=1)[:, None, :]
    big = np.kron(outer, np.eye(items, dtype=np.float32))
    y = mul(big, blocks.astype(jnp.float32).reshape(parts * items, cols))
    y = y.reshape(2, parts, items, cols)
    y = jnp.concatenate([y[0] * tw_c + y[1] * tw_s, y[1] * tw_c - y[0] * tw_s], axis=2)
    z = mul(y.reshape(parts * items, 2 * cols), inner)
    z = (z.reshape(parts, items, 2 * half) * weights).reshape(parts * items, 2 * half)
    v = mul(z, inner.T).reshape(parts, items, 2, cols)
    re, im = v[:, :, 0], v[:, :, 1]
    v = jnp.stack([re * tw_c - im * tw_s, im * tw_c + re * tw_s])
    return mul(big.T, v.reshape(2 * parts * items, cols)).reshape(parts, items, cols)


def dx(q):
    return 0.5 * (jnp.roll(q, -1, axis=-1) - jnp.roll(q, 1, axis=-1))


def dy(q):
    padded = jnp.pad(q, ((1, 1), (0, 0)))
    return 0.5 * (padded[2:] - padded[:-2])


def model_step(state, rotation):
    h, u, w = state
    h = h - COURANT * (dx(u) + dy(w))
    return h, u - COURANT * dx(h) + rotation * w, w - COURANT * dy(h) - rotation * u


def adjoint_step(state, rotation):
    h, u, w = state
    a = h + COURANT * (dx(u) + dy(w))
    return a, u - rotation * w + COURANT * dx(a), w + rotation * u + COURANT * dy(a)


HALO = 8


def widen(block):
    count = lax.axis_size("sp")
    up = [(i, (i + 1) % count) for i in range(count)]
    down = [(b, a) for a, b in up]
    low = lax.ppermute(block[..., -HALO:], "sp", up)
    high = lax.ppermute(block[..., :HALO], "sp", down)
    return jnp.concatenate([low, block, high], axis=-1)


def split2(x):
    hi = x.astype(jnp.bfloat16)
    return hi, (x - hi.astype(jnp.float32)).astype(jnp.bfloat16)


def per_device(alpha, ensemble, static_std, control, loc_spectrum, obs_cell, obs_step, innovation, obs_weight):
    members, rows, cols = alpha.shape
    groups, parts = lax.axis_size("grp"), lax.axis_size("sp")
    spread = 1.0 / math.sqrt(members * groups - 1)
    tile_rows = control.shape[1]
    own = rows // parts
    first_row = lax.axis_index("grp") * tile_rows
    first_col = lax.axis_index("sp") * cols

    def localize(fields):
        sent = fields.astype(jnp.bfloat16).transpose(1, 0, 2)
        got = lax.all_to_all(sent, "sp", 0, 0, tiled=True)
        out = spectral_filter(got.reshape(parts, own * members, cols), loc_spectrum)
        out = out.astype(jnp.bfloat16).reshape(rows, members, cols)
        return lax.all_to_all(out, "sp", 0, 0, tiled=True).transpose(1, 0, 2)

    localized = localize(alpha).astype(jnp.float32)
    partial = jnp.sum(ensemble.astype(jnp.float32) * localized[:, None], axis=0)
    base = jnp.zeros((3, rows, cols), jnp.float32)
    base = lax.dynamic_update_slice(base, static_std * control, (0, first_row, 0))
    increment = lax.psum(base + spread * partial, "grp")
    rotation = (0.1 + 0.2 * (jnp.arange(rows, dtype=jnp.float32) + 0.5) / rows)[:, None]
    state0 = tuple(widen(increment))
    state1 = model_step(state0, rotation)
    state2 = model_step(state1, rotation)
    heights = jnp.stack([s[0] for s in (state0, state1, state2)])[..., HALO:-HALO]
    heights = lax.dynamic_slice_in_dim(heights, first_row, tile_rows, axis=1)
    heights = heights.reshape(3 * tile_rows, cols)
    row = obs_cell // (cols * parts) - first_row
    col = obs_cell % (cols * parts) - first_col
    in_col = (col[:, None] == jnp.arange(cols)).astype(jnp.bfloat16)
    in_row = (obs_step * tile_rows + row)[:, None] == jnp.arange(3 * tile_rows)
    picked = jnp.dot(in_col, jnp.concatenate(split2(heights)).T, preferred_element_type=jnp.float32)
    picked = picked[:, : 3 * tile_rows] + picked[:, 3 * tile_rows :]
    observed = jnp.sum(jnp.where(in_row, picked, 0.0), axis=1)
    misfit = obs_weight * (observed - innovation)
    placed = jnp.where(in_row, misfit[:, None], 0.0)
    forcing = jnp.dot(jnp.concatenate(split2(placed), axis=1).T, in_col, preferred_element_type=jnp.float32)
    forcing = (forcing[: 3 * tile_rows] + forcing[3 * tile_rows :]).reshape(3, tile_rows, cols)
    forcing = widen(lax.all_gather(forcing, "grp", axis=1, tiled=True))
    zero = jnp.zeros_like(forcing[0])
    h, u, w = adjoint_step((forcing[2], zero, zero), rotation)
    h, u, w = adjoint_step((h + forcing[1], u, w), rotation)
    adjoint = jnp.stack([h + forcing[0], u, w])[..., HALO:-HALO]
    tile = lax.dynamic_slice_in_dim(adjoint, first_row, tile_rows, axis=1)
    grad_control = control + static_std * tile
    half = adjoint.astype(jnp.bfloat16).astype(jnp.float32)
    weighted = jnp.sum(ensemble.astype(jnp.float32) * half[None], axis=1)
    grad_alpha = alpha + spread * localize(weighted).astype(jnp.float32)
    return grad_alpha, grad_control


def solution(mesh):
    flat = P(("grp", "sp"))
    tile = P(None, "grp", "sp")
    return jax.shard_map(
        per_device,
        mesh=mesh,
        in_specs=(P("grp", None, "sp"), P("grp", None, None, "sp"), tile, tile, P(), flat, flat, flat, flat),
        out_specs=(P("grp", None, "sp"), tile),
        check_vma=False,
    )
```

```python
import functools
import math

import jax
import jax.numpy as jnp
import numpy as np
from jax import lax
from jax.experimental import pallas as pl
from jax.experimental.pallas import tpu as pltpu
from jax.sharding import PartitionSpec as P

COURANT = 0.4


def tables(parts, cols, waves):
    length = parts * cols
    inner_waves = waves // parts
    k1 = np.arange(parts)
    turn = 2 * np.pi * (np.outer(k1, np.arange(parts)) % parts) / parts
    outer = np.concatenate([np.cos(turn), -np.sin(turn)])
    twist = 2 * np.pi * np.outer(k1, np.arange(cols)) / length
    phase = 2 * np.pi * (np.outer(np.arange(cols), np.arange(inner_waves)) % cols) / cols
    c, s = np.cos(phase), np.sin(phase)
    inner = np.block([[c, -s], [s, c]])
    return [np.asarray(t, np.float32) for t in (outer, np.cos(twist), np.sin(twist), inner)]


EDGE = 128
BF16, F32 = jnp.bfloat16, jnp.float32


def dot(a, b, contract=((1,), (0,))):
    return lax.dot_general(a, b, (contract, ((), ())), preferred_element_type=F32)


def split2(x):
    hi = x.astype(BF16)
    return hi, (x - hi.astype(F32)).astype(BF16)


def right_mul(x, hi, lo):
    x_hi, x_lo = split2(x)
    return dot(x_hi, hi) + dot(x_lo, hi) + dot(x_hi, lo)


def left_mul(hi, lo, x):
    x_hi, x_lo = split2(x)
    return dot(hi, x_hi) + dot(hi, x_lo) + dot(lo, x_hi)


def dx(q):
    width = q.shape[1]
    return 0.5 * (pltpu.roll(q, width - 1, 1) - pltpu.roll(q, 1, 1))


def dy(q):
    rows = q.shape[0]
    at = lax.broadcasted_iota(jnp.int32, q.shape, 0)
    above = jnp.where(at < rows - 1, pltpu.roll(q, rows - 1, 0), 0.0)
    below = jnp.where(at > 0, pltpu.roll(q, 1, 0), 0.0)
    return 0.5 * (above - below)


def model_step(state, rotation):
    h, u, w = state
    h = h - COURANT * (dx(u) + dy(w))
    return h, u - COURANT * dx(h) + rotation * w, w - COURANT * dy(h) - rotation * u


def adjoint_step(state, rotation):
    h, u, w = state
    a = h + COURANT * (dx(u) + dy(w))
    return a, u - rotation * w + COURANT * dx(a), w + rotation * u + COURANT * dy(a)


def kernel(
    groups, parts, spread,
    alpha_ref, ens_ref, base_ref, weights_ref, tw_c_ref, tw_s_ref,
    big_hi, big_lo, bigt_hi, bigt_lo, in_hi, in_lo, int_hi, int_lo,
    col_ref, slot_ref, innovation_ref, obs_weight_ref,
    filtered_ref, adjoint_ref,
    snd, rcv, ex_src, ex_full, ex_low, ex_high,
    send_sem, recv_sem, ex_send, ex_recv,
):
    group, part = lax.axis_index("grp"), lax.axis_index("sp")
    left, right = lax.rem(part + parts - 1, parts), lax.rem(part + 1, parts)
    _, rows, cols = base_ref.shape
    own, padded = rows // parts, alpha_ref.shape[2]
    items = parts * own * padded

    barrier = pltpu.get_barrier_semaphore()
    for i in range(1, parts):
        pl.semaphore_signal(barrier, inc=1, device_id={"sp": lax.rem(part + i, parts)})
    for i in range(1, groups):
        for at in (left, part, right):
            pl.semaphore_signal(barrier, inc=1, device_id={"grp": lax.rem(group + i, groups), "sp": at})
    pl.semaphore_wait(barrier, parts - 1 + 3 * (groups - 1))

    def all_to_all(phase, source):
        copies = []
        for i in range(1, parts):
            to = lax.rem(part + i, parts)
            copies.append(pltpu.make_async_remote_copy(
                src_ref=source.at[to], dst_ref=rcv.at[phase, part],
                send_sem=send_sem.at[phase, i], recv_sem=recv_sem.at[phase, i],
                device_id={"sp": to},
            ))
            copies[-1].start()
        rcv[phase, part] = source[part]
        return copies

    def finish(copies):
        for copy in copies:
            copy.wait_recv()
        for copy in copies:
            copy.wait_send()

    def filtered(phase):
        x = rcv[phase].reshape(items, cols)
        c, s = tw_c_ref[...], tw_s_ref[...]
        y = dot(big_hi[...], x) + dot(big_lo[...], x)
        re, im = y[:items], y[items:]
        z = right_mul(re * c + im * s, in_hi[:cols], in_lo[:cols])
        z = z + right_mul(im * c - re * s, in_hi[cols:], in_lo[cols:])
        v = right_mul(z * weights_ref[...], int_hi[...], int_lo[...])
        re, im = v[:, :cols], v[:, cols:]
        out = left_mul(bigt_hi[:, :items], bigt_lo[:, :items], re * c - im * s)
        out = out + left_mul(bigt_hi[:, items:], bigt_lo[:, items:], im * c + re * s)
        return out.astype(BF16).reshape(parts, own, padded, cols)

    def exchange(step, fields):
        for v in range(3):
            ex_src[step, v] = fields[v]
        copies = []
        first, last = pl.ds(0, EDGE), pl.ds(cols - EDGE, EDGE)
        for i in range(groups):
            to = lax.rem(group + i, groups)
            plans = [(1, right, ex_src.at[step, :, :, last], ex_low), (2, left, ex_src.at[step, :, :, first], ex_high)]
            if i > 0:
                plans.append((0, part, ex_src.at[step], ex_full))
            for kind, at, source, target in plans:
                copies.append(pltpu.make_async_remote_copy(
                    src_ref=source, dst_ref=target.at[step, group],
                    send_sem=ex_send.at[step, kind, i], recv_sem=ex_recv.at[step, kind, i],
                    device_id={"grp": to, "sp": at},
                ))
                copies[-1].start()
        ex_full[step, group] = ex_src[step]
        finish(copies)
        wide = []
        for v in range(3):
            pieces = []
            for buffer in (ex_low, ex_full, ex_high):
                total = buffer[step, 0, v]
                for g in range(1, groups):
                    total = total + buffer[step, g, v]
                pieces.append(total)
            wide.append(jnp.concatenate(pieces, axis=1))
        return wide

    copies = all_to_all(0, alpha_ref)
    in_col = (lax.broadcasted_iota(jnp.int32, (cols, col_ref.shape[1]), 0) == col_ref[...]).astype(F32).astype(BF16)
    in_slot = lax.broadcasted_iota(jnp.int32, (3 * rows, col_ref.shape[1]), 0) == slot_ref[...]
    finish(copies)
    snd[0] = filtered(0)
    finish(all_to_all(1, snd.at[0]))
    localized = rcv[1].reshape(rows, padded, cols).astype(F32)
    partial = [base_ref[v] + spread * jnp.sum(ens_ref[v].astype(F32) * localized, axis=1) for v in range(3)]
    state0 = exchange(0, partial)
    row_at = lax.broadcasted_iota(jnp.int32, (rows, cols + 2 * EDGE), 0).astype(F32)
    rotation = 0.1 + 0.2 * (row_at + 0.5) / rows
    state1 = model_step(state0, rotation)
    state2 = model_step(state1, rotation)
    heights = jnp.concatenate([s[0][:, EDGE:-EDGE] for s in (state0, state1, state2)], axis=0)
    high, low = split2(heights)
    picked = dot(high, in_col) + dot(low, in_col)
    observed = jnp.sum(jnp.where(in_slot, picked, 0.0), axis=0, keepdims=True)
    misfit = obs_weight_ref[...] * (observed - innovation_ref[...])
    high, low = split2(jnp.where(in_slot, misfit, 0.0))
    forcing = dot(high, in_col, ((1,), (1,))) + dot(low, in_col, ((1,), (1,)))
    forcing = exchange(1, [forcing[t * rows : (t + 1) * rows] for t in range(3)])
    zero = jnp.zeros_like(rotation)
    h, u, w = adjoint_step((forcing[2], zero, zero), rotation)
    h, u, w = adjoint_step((h + forcing[1], u, w), rotation)
    weighted = jnp.zeros((rows, padded, cols), F32)
    for v, field in enumerate((h + forcing[0], u, w)):
        field = field[:, EDGE:-EDGE]
        adjoint_ref[v] = field
        half = field.astype(BF16).astype(F32)
        weighted = weighted + ens_ref[v].astype(F32) * half[:, None, :]
    snd[1] = weighted.astype(BF16).reshape(parts, own, padded, cols)
    finish(all_to_all(2, snd.at[1]))
    snd[2] = filtered(2)
    finish(all_to_all(3, snd.at[2]))
    filtered_ref[...] = rcv[3].reshape(rows, padded, cols)


def both(table):
    hi = table.astype(BF16)
    return hi, (table - hi.astype(np.float32)).astype(BF16)


def per_device(alpha, ensemble, static_std, control, loc_spectrum, obs_cell, obs_step, innovation, obs_weight):
    members, rows, cols = alpha.shape
    groups, parts = lax.axis_size("grp"), lax.axis_size("sp")
    spread = 1.0 / math.sqrt(members * groups - 1)
    tile_rows, own = control.shape[1], rows // parts
    padded = -(-members // 16) * 16
    first_row = lax.axis_index("grp") * tile_rows
    first_col = lax.axis_index("sp") * cols
    fill = padded - members

    outer, tw_c, tw_s, inner = tables(parts, cols, loc_spectrum.shape[0])
    items = own * padded
    big = np.kron(outer, np.eye(items, dtype=np.float32))
    waves = loc_spectrum.reshape(inner.shape[1] // 2, parts).T
    waves = jnp.repeat(jnp.concatenate([waves, waves], axis=1), items, axis=0)
    sent = jnp.pad(alpha.astype(BF16).transpose(1, 0, 2), ((0, 0), (0, fill), (0, 0)))
    ens = jnp.pad(ensemble.transpose(1, 2, 0, 3), ((0, 0), (0, 0), (0, fill), (0, 0)))
    base = jnp.zeros((3, rows, cols), F32)
    base = lax.dynamic_update_slice(base, static_std * control, (0, first_row, 0))
    col = obs_cell % (cols * parts) - first_col
    slot = obs_step * rows + obs_cell // (cols * parts)
    vmem = pl.BlockSpec(memory_space=pltpu.VMEM)
    operands = (
        sent.reshape(parts, own, padded, cols), ens, base, waves,
        np.repeat(tw_c, items, axis=0), np.repeat(tw_s, items, axis=0),
        *both(big), *both(big.T), *both(inner), *both(inner.T),
        col[None], slot[None], innovation[None], obs_weight[None],
    )
    filtered, adjoint = pl.pallas_call(
        functools.partial(kernel, groups, parts, spread),
        out_shape=(
            jax.ShapeDtypeStruct((rows, padded, cols), BF16),
            jax.ShapeDtypeStruct((3, rows, cols), F32),
        ),
        in_specs=[vmem] * len(operands),
        out_specs=(vmem, vmem),
        scratch_shapes=[
            pltpu.VMEM((3, parts, own, padded, cols), BF16),
            pltpu.VMEM((4, parts, own, padded, cols), BF16),
            pltpu.VMEM((2, 3, rows, cols), F32),
            pltpu.VMEM((2, groups, 3, rows, cols), F32),
            pltpu.VMEM((2, groups, 3, rows, EDGE), F32),
            pltpu.VMEM((2, groups, 3, rows, EDGE), F32),
            pltpu.SemaphoreType.DMA((4, parts)),
            pltpu.SemaphoreType.DMA((4, parts)),
            pltpu.SemaphoreType.DMA((2, 3, groups)),
            pltpu.SemaphoreType.DMA((2, 3, groups)),
        ],
        compiler_params=pltpu.CompilerParams(collective_id=0, has_side_effects=True, vmem_limit_bytes=60 << 20),
    )(*operands)
    filtered = filtered[:, :members].transpose(1, 0, 2).astype(F32)
    grad_alpha = alpha + spread * filtered
    tile = lax.dynamic_slice_in_dim(adjoint, first_row, tile_rows, axis=1)
    return grad_alpha, control + static_std * tile


def solution(mesh):
    flat = P(("grp", "sp"))
    tile = P(None, "grp", "sp")
    return jax.shard_map(
        per_device,
        mesh=mesh,
        in_specs=(P("grp", None, "sp"), P("grp", None, None, "sp"), tile, tile, P(), flat, flat, flat, flat),
        out_specs=(P("grp", None, "sp"), tile),
        check_vma=False,
    )
```

```python
import functools
import math

import jax
import jax.numpy as jnp
import numpy as np
from jax import lax
from jax.experimental import pallas as pl
from jax.experimental.pallas import tpu as pltpu
from jax.sharding import PartitionSpec as P

COURANT = 0.4


def tables(parts, cols, waves):
    length = parts * cols
    inner_waves = waves // parts
    k1 = np.arange(parts)
    turn = 2 * np.pi * (np.outer(k1, np.arange(parts)) % parts) / parts
    outer = np.concatenate([np.cos(turn), -np.sin(turn)])
    twist = 2 * np.pi * np.outer(k1, np.arange(cols)) / length
    phase = 2 * np.pi * (np.outer(np.arange(cols), np.arange(inner_waves)) % cols) / cols
    c, s = np.cos(phase), np.sin(phase)
    inner = np.block([[c, -s], [s, c]])
    return [np.asarray(t, np.float32) for t in (outer, np.cos(twist), np.sin(twist), inner)]


EDGE = 128
BF16, F32 = jnp.bfloat16, jnp.float32


def dot(a, b, contract=((1,), (0,))):
    return lax.dot_general(a, b, (contract, ((), ())), preferred_element_type=F32)


def split2(x):
    hi = x.astype(BF16)
    return hi, (x - hi.astype(F32)).astype(BF16)


def right_mul(x, hi, lo):
    x_hi, x_lo = split2(x)
    return dot(x_hi, hi) + dot(x_lo, hi) + dot(x_hi, lo)


def left_mul(hi, lo, x):
    x_hi, x_lo = split2(x)
    return dot(hi, x_hi) + dot(hi, x_lo) + dot(lo, x_hi)


def dx(q):
    width = q.shape[1]
    return 0.5 * (pltpu.roll(q, width - 1, 1) - pltpu.roll(q, 1, 1))


def dy(q):
    rows = q.shape[0]
    at = lax.broadcasted_iota(jnp.int32, q.shape, 0)
    above = jnp.where(at < rows - 1, pltpu.roll(q, rows - 1, 0), 0.0)
    below = jnp.where(at > 0, pltpu.roll(q, 1, 0), 0.0)
    return 0.5 * (above - below)


def model_step(state, rotation):
    h, u, w = state
    h = h - COURANT * (dx(u) + dy(w))
    return h, u - COURANT * dx(h) + rotation * w, w - COURANT * dy(h) - rotation * u


def adjoint_step(state, rotation):
    h, u, w = state
    a = h + COURANT * (dx(u) + dy(w))
    return a, u - rotation * w + COURANT * dx(a), w + rotation * u + COURANT * dy(a)


def kernel(
    groups, parts, spread,
    alpha_ref, ensemble_ref, std_ref, control_ref, weights_ref, tw_c_ref, tw_s_ref,
    big_hi, big_lo, bigt_hi, bigt_lo, in_hi, in_lo, int_hi, int_lo,
    cell_ref, step_ref, innovation_ref, obs_weight_ref,
    grad_alpha_ref, grad_control_ref,
    stage, ens, adjoint, snd, rcv, ex_src, ex_full, ex_low, ex_high,
    send_sem, recv_sem, ex_send, ex_recv,
):
    group, part = lax.axis_index("grp"), lax.axis_index("sp")
    left, right = lax.rem(part + parts - 1, parts), lax.rem(part + 1, parts)
    members, rows, cols = alpha_ref.shape
    own, padded = rows // parts, stage.shape[1]
    tile_rows = control_ref.shape[1]
    tile = pl.ds(pl.multiple_of(group * tile_rows, tile_rows), tile_rows)
    items = parts * own * padded

    barrier = pltpu.get_barrier_semaphore()
    for i in range(1, parts):
        pl.semaphore_signal(barrier, inc=1, device_id={"sp": lax.rem(part + i, parts)})
    for i in range(1, groups):
        for at in (left, part, right):
            pl.semaphore_signal(barrier, inc=1, device_id={"grp": lax.rem(group + i, groups), "sp": at})

    if padded > members:
        stage[:, members:, :] = jnp.zeros((rows, padded - members, cols), F32)
        for v in range(3):
            ens[v, :, members:, :] = jnp.zeros((rows, padded - members, cols), F32)
    for m in range(members):
        stage[:, m, :] = alpha_ref[m]
    snd[0] = stage[...].astype(BF16).reshape(parts, own, padded, cols)
    cell = cell_ref[...]
    row = jnp.zeros_like(cell)
    for r in range(1, rows):
        row = row + jnp.where(cell >= r * cols * parts, 1, 0)
    col = cell - row * (cols * parts) - part * cols
    slot = step_ref[...] * rows + row
    in_col = (lax.broadcasted_iota(jnp.int32, (cols, cell.shape[1]), 0) == col).astype(F32).astype(BF16)
    in_slot = lax.broadcasted_iota(jnp.int32, (3 * rows, cell.shape[1]), 0) == slot
    pl.semaphore_wait(barrier, parts - 1 + 3 * (groups - 1))
    started = []
    waves = jnp.broadcast_to(weights_ref[...][:, None, :], (parts, own * padded, weights_ref.shape[1]))
    waves = waves.reshape(items, weights_ref.shape[1])

    def all_to_all(phase, source):
        copies = []
        for i in range(1, parts):
            to = lax.rem(part + i, parts)
            copies.append(pltpu.make_async_remote_copy(
                src_ref=source.at[to], dst_ref=rcv.at[phase, part],
                send_sem=send_sem.at[phase, i], recv_sem=recv_sem.at[phase, i],
                device_id={"sp": to},
            ))
            copies[-1].start()
        rcv[phase, part] = source[part]
        return copies

    def finish(copies):
        for copy in copies:
            copy.wait_recv()
        started.extend(copies)

    def filtered(phase):
        x = rcv[phase].reshape(items, cols)
        c, s = tw_c_ref[...], tw_s_ref[...]
        y = dot(big_hi[...], x) + dot(big_lo[...], x)
        re, im = y[:items], y[items:]
        z = right_mul(re * c + im * s, in_hi[:cols], in_lo[:cols])
        z = z + right_mul(im * c - re * s, in_hi[cols:], in_lo[cols:])
        v = right_mul(z * waves, int_hi[...], int_lo[...])
        re, im = v[:, :cols], v[:, cols:]
        out = left_mul(bigt_hi[:, :items], bigt_lo[:, :items], re * c - im * s)
        out = out + left_mul(bigt_hi[:, items:], bigt_lo[:, items:], im * c + re * s)
        return out.astype(BF16).reshape(parts, own, padded, cols)

    def exchange(step):
        copies = []
        first, last = pl.ds(0, EDGE), pl.ds(cols - EDGE, EDGE)
        for i in range(groups):
            to = lax.rem(group + i, groups)
            plans = [(1, right, ex_src.at[step, :, :, last], ex_low), (2, left, ex_src.at[step, :, :, first], ex_high)]
            if i > 0:
                plans.append((0, part, ex_src.at[step], ex_full))
            for kind, at, source, target in plans:
                copies.append(pltpu.make_async_remote_copy(
                    src_ref=source, dst_ref=target.at[step, group],
                    send_sem=ex_send.at[step, kind, i], recv_sem=ex_recv.at[step, kind, i],
                    device_id={"grp": to, "sp": at},
                ))
                copies[-1].start()
        ex_full[step, group] = ex_src[step]
        finish(copies)
        wide = []
        for v in range(3):
            pieces = []
            for buffer in (ex_low, ex_full, ex_high):
                total = buffer[step, 0, v]
                for g in range(1, groups):
                    total = total + buffer[step, g, v]
                pieces.append(total)
            wide.append(jnp.concatenate(pieces, axis=1))
        return wide

    copies = all_to_all(0, snd.at[0])
    for m in range(members):
        for v in range(3):
            ens[v, :, m, :] = ensemble_ref[m, v].astype(F32)
    finish(copies)
    snd[1] = filtered(0)
    finish(all_to_all(1, snd.at[1]))
    localized = rcv[1].reshape(rows, padded, cols).astype(F32)
    for v in range(3):
        ex_src[0, v] = spread * jnp.sum(ens[v] * localized, axis=1)
        ex_src[0, v, tile, :] = ex_src[0, v, tile, :] + std_ref[v] * control_ref[v]
    state0 = exchange(0)
    row_at = lax.broadcasted_iota(jnp.int32, (rows, cols + 2 * EDGE), 0).astype(F32)
    rotation = 0.1 + 0.2 * (row_at + 0.5) / rows
    state1 = model_step(state0, rotation)
    state2 = model_step(state1, rotation)
    heights = jnp.concatenate([s[0][:, EDGE:-EDGE] for s in (state0, state1, state2)], axis=0)
    high, low = split2(heights)
    picked = dot(high, in_col) + dot(low, in_col)
    observed = jnp.sum(jnp.where(in_slot, picked, 0.0), axis=0, keepdims=True)
    misfit = obs_weight_ref[...] * (observed - innovation_ref[...])
    high, low = split2(jnp.where(in_slot, misfit, 0.0))
    forcing = dot(high, in_col, ((1,), (1,))) + dot(low, in_col, ((1,), (1,)))
    for t in range(3):
        ex_src[1, t] = forcing[t * rows : (t + 1) * rows]
    forcing = exchange(1)
    zero = jnp.zeros_like(rotation)
    h, u, w = adjoint_step((forcing[2], zero, zero), rotation)
    h, u, w = adjoint_step((h + forcing[1], u, w), rotation)
    weighted = jnp.zeros((rows, padded, cols), F32)
    for v, field in enumerate((h + forcing[0], u, w)):
        field = field[:, EDGE:-EDGE]
        adjoint[v] = field
        half = field.astype(BF16).astype(F32)
        weighted = weighted + ens[v] * half[:, None, :]
    snd[2] = weighted.astype(BF16).reshape(parts, own, padded, cols)
    copies = all_to_all(2, snd.at[2])
    for v in range(3):
        grad_control_ref[v] = control_ref[v] + std_ref[v] * adjoint[v, tile, :]
    finish(copies)
    snd[3] = filtered(2)
    finish(all_to_all(3, snd.at[3]))
    stage[...] = rcv[3].reshape(rows, padded, cols).astype(F32)
    for m in range(members):
        grad_alpha_ref[m] = alpha_ref[m] + spread * stage[:, m, :]
    for copy in started:
        copy.wait_send()


def both(table):
    hi = table.astype(BF16)
    return hi, (table - hi.astype(np.float32)).astype(BF16)


def per_device(alpha, ensemble, static_std, control, loc_spectrum, obs_cell, obs_step, innovation, obs_weight):
    members, rows, cols = alpha.shape
    groups, parts = lax.axis_size("grp"), lax.axis_size("sp")
    spread = 1.0 / math.sqrt(members * groups - 1)
    own = rows // parts
    padded = -(-members // 16) * 16

    outer, tw_c, tw_s, inner = tables(parts, cols, loc_spectrum.shape[0])
    items = own * padded
    big = np.kron(outer, np.eye(items, dtype=np.float32))
    waves = loc_spectrum.reshape(inner.shape[1] // 2, parts).T
    waves = jnp.concatenate([waves, waves], axis=1)
    vmem = pl.BlockSpec(memory_space=pltpu.VMEM)
    operands = (
        alpha, ensemble, static_std, control, waves,
        np.repeat(tw_c, items, axis=0), np.repeat(tw_s, items, axis=0),
        *both(big), *both(big.T), *both(inner), *both(inner.T),
        obs_cell[None], obs_step[None], innovation[None], obs_weight[None],
    )
    return pl.pallas_call(
        functools.partial(kernel, groups, parts, spread),
        out_shape=(
            jax.ShapeDtypeStruct(alpha.shape, F32),
            jax.ShapeDtypeStruct(control.shape, F32),
        ),
        in_specs=[vmem] * len(operands),
        out_specs=(vmem, vmem),
        scratch_shapes=[
            pltpu.VMEM((rows, padded, cols), F32),
            pltpu.VMEM((3, rows, padded, cols), F32),
            pltpu.VMEM((3, rows, cols), F32),
            pltpu.VMEM((4, parts, own, padded, cols), BF16),
            pltpu.VMEM((4, parts, own, padded, cols), BF16),
            pltpu.VMEM((2, 3, rows, cols), F32),
            pltpu.VMEM((2, groups, 3, rows, cols), F32),
            pltpu.VMEM((2, groups, 3, rows, EDGE), F32),
            pltpu.VMEM((2, groups, 3, rows, EDGE), F32),
            pltpu.SemaphoreType.DMA((4, parts)),
            pltpu.SemaphoreType.DMA((4, parts)),
            pltpu.SemaphoreType.DMA((2, 3, groups)),
            pltpu.SemaphoreType.DMA((2, 3, groups)),
        ],
        compiler_params=pltpu.CompilerParams(collective_id=0, has_side_effects=True, vmem_limit_bytes=60 << 20),
    )(*operands)


def solution(mesh):
    flat = P(("grp", "sp"))
    tile = P(None, "grp", "sp")
    return jax.shard_map(
        per_device,
        mesh=mesh,
        in_specs=(P("grp", None, "sp"), P("grp", None, None, "sp"), tile, tile, P(), flat, flat, flat, flat),
        out_specs=(P("grp", None, "sp"), tile),
        check_vma=False,
    )
```

```python
import functools
import math

import jax
import jax.numpy as jnp
import numpy as np
from jax import lax
from jax.experimental import pallas as pl
from jax.experimental.pallas import tpu as pltpu
from jax.sharding import PartitionSpec as P

COURANT = 0.4


def tables(parts, cols, waves):
    length = parts * cols
    inner_waves = waves // parts
    k1 = np.arange(parts)
    turn = 2 * np.pi * (np.outer(k1, np.arange(parts)) % parts) / parts
    outer = np.concatenate([np.cos(turn), -np.sin(turn)])
    twist = 2 * np.pi * np.outer(k1, np.arange(cols)) / length
    phase = 2 * np.pi * (np.outer(np.arange(cols), np.arange(inner_waves)) % cols) / cols
    c, s = np.cos(phase), np.sin(phase)
    inner = np.block([[c, -s], [s, c]])
    return [np.asarray(t, np.float32) for t in (outer, np.cos(twist), np.sin(twist), inner)]


EDGE = 128
BF16, F32 = jnp.bfloat16, jnp.float32


def dot(a, b, contract=((1,), (0,))):
    return lax.dot_general(a, b, (contract, ((), ())), preferred_element_type=F32)


def split2(x):
    hi = x.astype(BF16)
    return hi, (x - hi.astype(F32)).astype(BF16)


def right_mul(x, hi, lo):
    x_hi, x_lo = split2(x)
    return dot(x_hi, hi) + dot(x_lo, hi) + dot(x_hi, lo)


def left_mul(hi, lo, x):
    x_hi, x_lo = split2(x)
    return dot(hi, x_hi) + dot(hi, x_lo) + dot(lo, x_hi)


def dx(q):
    width = q.shape[1]
    return 0.5 * (pltpu.roll(q, width - 1, 1) - pltpu.roll(q, 1, 1))


def dy(q):
    rows = q.shape[0]
    at = lax.broadcasted_iota(jnp.int32, q.shape, 0)
    above = jnp.where(at < rows - 1, pltpu.roll(q, rows - 1, 0), 0.0)
    below = jnp.where(at > 0, pltpu.roll(q, 1, 0), 0.0)
    return 0.5 * (above - below)


def model_step(state, rotation):
    h, u, w = state
    h = h - COURANT * (dx(u) + dy(w))
    return h, u - COURANT * dx(h) + rotation * w, w - COURANT * dy(h) - rotation * u


def adjoint_step(state, rotation):
    h, u, w = state
    a = h + COURANT * (dx(u) + dy(w))
    return a, u - rotation * w + COURANT * dx(a), w + rotation * u + COURANT * dy(a)


def kernel(
    groups, parts, spread,
    alpha_ref, std_ref, control_ref, weights_ref,
    cell_ref, step_ref, innovation_ref, obs_weight_ref, *refs,
):
    far, near = refs[:11], refs[13:24]
    kernel_body(groups, parts, spread, alpha_ref, std_ref, control_ref, weights_ref, cell_ref, step_ref,
                innovation_ref, obs_weight_ref, far, near, *near, *refs[11:13], *refs[24:])


def kernel_body(
    groups, parts, spread,
    alpha_ref, std_ref, control_ref, weights_ref,
    cell_ref, step_ref, innovation_ref, obs_weight_ref, far, near,
    ensemble_ref, tw_c_ref, tw_s_ref,
    big_hi, big_lo, bigt_hi, bigt_lo, in_hi, in_lo, int_hi, int_lo,
    grad_alpha_ref, grad_control_ref,
    stage, ens, adjoint, snd, rcv, ex_src, ex_full, ex_low, ex_high,
    send_sem, recv_sem, ex_send, ex_recv, load_sem,
):
    group, part = lax.axis_index("grp"), lax.axis_index("sp")
    left, right = lax.rem(part + parts - 1, parts), lax.rem(part + 1, parts)
    members, rows, cols = alpha_ref.shape
    own, padded = rows // parts, stage.shape[1]
    tile_rows = control_ref.shape[1]
    tile = pl.ds(pl.multiple_of(group * tile_rows, tile_rows), tile_rows)
    items = parts * own * padded

    barrier = pltpu.get_barrier_semaphore()
    for i in range(1, parts):
        pl.semaphore_signal(barrier, inc=1, device_id={"sp": lax.rem(part + i, parts)})
    for i in range(1, groups):
        for at in (left, part, right):
            pl.semaphore_signal(barrier, inc=1, device_id={"grp": lax.rem(group + i, groups), "sp": at})

    loads = [pltpu.make_async_copy(a, b, load_sem.at[i]) for i, (a, b) in enumerate(zip(far, near))]
    for load in loads:
        load.start()
    if padded > members:
        stage[:, members:, :] = jnp.zeros((rows, padded - members, cols), F32)
        for v in range(3):
            ens[v, :, members:, :] = jnp.zeros((rows, padded - members, cols), F32)
    for m in range(members):
        stage[:, m, :] = alpha_ref[m]
    snd[0] = stage[...].astype(BF16).reshape(parts, own, padded, cols)
    cell = cell_ref[...]
    row = jnp.zeros_like(cell)
    for r in range(1, rows):
        row = row + jnp.where(cell >= r * cols * parts, 1, 0)
    col = cell - row * (cols * parts) - part * cols
    slot = step_ref[...] * rows + row
    in_col = (lax.broadcasted_iota(jnp.int32, (cols, cell.shape[1]), 0) == col).astype(F32).astype(BF16)
    in_slot = lax.broadcasted_iota(jnp.int32, (3 * rows, cell.shape[1]), 0) == slot
    pl.semaphore_wait(barrier, parts - 1 + 3 * (groups - 1))
    started = []
    waves = jnp.broadcast_to(weights_ref[...][:, None, :], (parts, own * padded, weights_ref.shape[1]))
    waves = waves.reshape(items, weights_ref.shape[1])

    def all_to_all(phase, source):
        copies = []
        for i in range(1, parts):
            to = lax.rem(part + i, parts)
            copies.append(pltpu.make_async_remote_copy(
                src_ref=source.at[to], dst_ref=rcv.at[phase, part],
                send_sem=send_sem.at[phase, i], recv_sem=recv_sem.at[phase, i],
                device_id={"sp": to},
            ))
            copies[-1].start()
        rcv[phase, part] = source[part]
        return copies

    def finish(copies):
        for copy in copies:
            copy.wait_recv()
        started.extend(copies)

    def filtered(phase):
        x = rcv[phase].reshape(items, cols)
        c, s = tw_c_ref[...], tw_s_ref[...]
        y = dot(big_hi[...], x) + dot(big_lo[...], x)
        re, im = y[:items], y[items:]
        z = right_mul(re * c + im * s, in_hi[:cols], in_lo[:cols])
        z = z + right_mul(im * c - re * s, in_hi[cols:], in_lo[cols:])
        v = right_mul(z * waves, int_hi[...], int_lo[...])
        re, im = v[:, :cols], v[:, cols:]
        out = left_mul(bigt_hi[:, :items], bigt_lo[:, :items], re * c - im * s)
        out = out + left_mul(bigt_hi[:, items:], bigt_lo[:, items:], im * c + re * s)
        return out.astype(BF16).reshape(parts, own, padded, cols)

    def exchange(step):
        copies = []
        first, last = pl.ds(0, EDGE), pl.ds(cols - EDGE, EDGE)
        for i in range(groups):
            to = lax.rem(group + i, groups)
            plans = [(1, right, ex_src.at[step, :, :, last], ex_low), (2, left, ex_src.at[step, :, :, first], ex_high)]
            if i > 0:
                plans.append((0, part, ex_src.at[step], ex_full))
            for kind, at, source, target in plans:
                copies.append(pltpu.make_async_remote_copy(
                    src_ref=source, dst_ref=target.at[step, group],
                    send_sem=ex_send.at[step, kind, i], recv_sem=ex_recv.at[step, kind, i],
                    device_id={"grp": to, "sp": at},
                ))
                copies[-1].start()
        ex_full[step, group] = ex_src[step]
        finish(copies)
        wide = []
        for v in range(3):
            pieces = []
            for buffer in (ex_low, ex_full, ex_high):
                total = buffer[step, 0, v]
                for g in range(1, groups):
                    total = total + buffer[step, g, v]
                pieces.append(total)
            wide.append(jnp.concatenate(pieces, axis=1))
        return wide

    copies = all_to_all(0, snd.at[0])
    loads[0].wait()
    for m in range(members):
        for v in range(3):
            ens[v, :, m, :] = ensemble_ref[m, v].astype(F32)
    for load in loads[1:]:
        load.wait()
    finish(copies)
    snd[1] = filtered(0)
    finish(all_to_all(1, snd.at[1]))
    localized = rcv[1].reshape(rows, padded, cols).astype(F32)
    for v in range(3):
        ex_src[0, v] = spread * jnp.sum(ens[v] * localized, axis=1)
        ex_src[0, v, tile, :] = ex_src[0, v, tile, :] + std_ref[v] * control_ref[v]
    state0 = exchange(0)
    row_at = lax.broadcasted_iota(jnp.int32, (rows, cols + 2 * EDGE), 0).astype(F32)
    rotation = 0.1 + 0.2 * (row_at + 0.5) / rows
    state1 = model_step(state0, rotation)
    state2 = model_step(state1, rotation)
    heights = jnp.concatenate([s[0][:, EDGE:-EDGE] for s in (state0, state1, state2)], axis=0)
    high, low = split2(heights)
    picked = dot(high, in_col) + dot(low, in_col)
    observed = jnp.sum(jnp.where(in_slot, picked, 0.0), axis=0, keepdims=True)
    misfit = obs_weight_ref[...] * (observed - innovation_ref[...])
    high, low = split2(jnp.where(in_slot, misfit, 0.0))
    forcing = dot(high, in_col, ((1,), (1,))) + dot(low, in_col, ((1,), (1,)))
    for t in range(3):
        ex_src[1, t] = forcing[t * rows : (t + 1) * rows]
    forcing = exchange(1)
    zero = jnp.zeros_like(rotation)
    h, u, w = adjoint_step((forcing[2], zero, zero), rotation)
    h, u, w = adjoint_step((h + forcing[1], u, w), rotation)
    weighted = jnp.zeros((rows, padded, cols), F32)
    for v, field in enumerate((h + forcing[0], u, w)):
        field = field[:, EDGE:-EDGE]
        adjoint[v] = field
        half = field.astype(BF16).astype(F32)
        weighted = weighted + ens[v] * half[:, None, :]
    snd[2] = weighted.astype(BF16).reshape(parts, own, padded, cols)
    copies = all_to_all(2, snd.at[2])
    for v in range(3):
        grad_control_ref[v] = control_ref[v] + std_ref[v] * adjoint[v, tile, :]
    finish(copies)
    snd[3] = filtered(2)
    finish(all_to_all(3, snd.at[3]))
    stage[...] = rcv[3].reshape(rows, padded, cols).astype(F32)
    for m in range(members):
        grad_alpha_ref[m] = alpha_ref[m] + spread * stage[:, m, :]
    for copy in started:
        copy.wait_send()


def both(table):
    hi = table.astype(BF16)
    return hi, (table - hi.astype(np.float32)).astype(BF16)


def per_device(alpha, ensemble, static_std, control, loc_spectrum, obs_cell, obs_step, innovation, obs_weight):
    members, rows, cols = alpha.shape
    groups, parts = lax.axis_size("grp"), lax.axis_size("sp")
    spread = 1.0 / math.sqrt(members * groups - 1)
    own = rows // parts
    padded = -(-members // 16) * 16

    outer, tw_c, tw_s, inner = tables(parts, cols, loc_spectrum.shape[0])
    items = own * padded
    big = np.kron(outer, np.eye(items, dtype=np.float32))
    waves = loc_spectrum.reshape(inner.shape[1] // 2, parts).T
    waves = jnp.concatenate([waves, waves], axis=1)
    vmem = pl.BlockSpec(memory_space=pltpu.VMEM)
    operands = (
        alpha, static_std, control, waves,
        obs_cell[None], obs_step[None], innovation[None], obs_weight[None],
    )
    loaded = (
        ensemble,
        np.repeat(tw_c, items, axis=0), np.repeat(tw_s, items, axis=0),
        *both(big), *both(big.T), *both(inner), *both(inner.T),
    )
    return pl.pallas_call(
        functools.partial(kernel, groups, parts, spread),
        out_shape=(
            jax.ShapeDtypeStruct(alpha.shape, F32),
            jax.ShapeDtypeStruct(control.shape, F32),
        ),
        in_specs=[vmem] * len(operands) + [pl.BlockSpec(memory_space=pl.ANY)] * len(loaded),
        out_specs=(vmem, vmem),
        scratch_shapes=[
            *[pltpu.VMEM(t.shape, t.dtype) for t in loaded],
            pltpu.VMEM((rows, padded, cols), F32),
            pltpu.VMEM((3, rows, padded, cols), F32),
            pltpu.VMEM((3, rows, cols), F32),
            pltpu.VMEM((4, parts, own, padded, cols), BF16),
            pltpu.VMEM((4, parts, own, padded, cols), BF16),
            pltpu.VMEM((2, 3, rows, cols), F32),
            pltpu.VMEM((2, groups, 3, rows, cols), F32),
            pltpu.VMEM((2, groups, 3, rows, EDGE), F32),
            pltpu.VMEM((2, groups, 3, rows, EDGE), F32),
            pltpu.SemaphoreType.DMA((4, parts)),
            pltpu.SemaphoreType.DMA((4, parts)),
            pltpu.SemaphoreType.DMA((2, 3, groups)),
            pltpu.SemaphoreType.DMA((2, 3, groups)),
            pltpu.SemaphoreType.DMA((len(loaded),)),
        ],
        compiler_params=pltpu.CompilerParams(collective_id=0, has_side_effects=True, vmem_limit_bytes=60 << 20),
    )(*operands, *loaded)


def solution(mesh):
    flat = P(("grp", "sp"))
    tile = P(None, "grp", "sp")
    return jax.shard_map(
        per_device,
        mesh=mesh,
        in_specs=(P("grp", None, "sp"), P("grp", None, None, "sp"), tile, tile, P(), flat, flat, flat, flat),
        out_specs=(P("grp", None, "sp"), tile),
        check_vma=False,
    )
```
